16 devices in a mesh: dp: 4 (over z, y), sp: 4 (over x, core).
Axes of the slice: x: 2, y: 2, z: 2, core: 2. Of those that a mesh axis runs over, the one named last changes fastest.
Arguments:
- latent: bfloat16 [64, 12, 48, 1280], P('dp', 'sp'), parts along dimension 0
- context: bfloat16 [64, 77, 2048], P('dp'), parts along dimension 0
- gn_gain: bfloat16 [1280], replicated
- gn_bias: bfloat16 [1280], replicated
- w_in: bfloat16 [1280, 1280], replicated
- b_in: bfloat16 [1280], replicated
- ln_gain: bfloat16 [2, 3, 1280], replicated
- ln_bias: bfloat16 [2, 3, 1280], replicated
- w_self: bfloat16 [2, 4, 1280, 1280], replicated
- b_self: bfloat16 [2, 1280], replicated
- w_cross_q: bfloat16 [2, 1280, 1280], replicated
- w_cross_kv: bfloat16 [2, 2, 2048, 1280], replicated
- w_cross_o: bfloat16 [2, 1280, 1280], replicated
- b_cross: bfloat16 [2, 1280], replicated
- w_ff1: bfloat16 [2, 1280, 10240], replicated
- b_ff1: bfloat16 [2, 10240], replicated
- w_ff2: bfloat16 [2, 5120, 1280], replicated
- b_ff2: bfloat16 [2, 1280], replicated
- w_out: bfloat16 [1280, 1280], replicated
- b_out: bfloat16 [1280], replicated
Outputs:
- output: bfloat16 [64, 12, 48, 1280], P('dp', 'sp'), parts along dimension 0
There are 4 independent parts. The reference program is written for one: setup_inputs(seed, part) draws one part's arguments, and reference() takes and returns one part's arrays. A program takes and returns all parts, laid end to end along the dimension named above; an argument that names none is the same for every part.
All inputs are finite; a program needn't handle non-finite values.
Results may differ from the reference program's by a relative error of at most 0.0129083.
Values are sent between devices in bfloat16 or wider.
A program may use at most 1 GiB of HBM per device.

```python
import jax
import jax.numpy as jnp
from jax import lax

BATCH_SIZE = 16
LAT_ROWS = 12
LAT_COLS = 48
CHANNELS = 1280
NUM_HEADS = 20
HEAD_DIM = 64
TEXT_LEN = 77
TEXT_DIM = 2048
FF_DIM = 5120
NUM_GROUPS = 32
NUM_LAYERS = 2


def draw_normal(key, shape, scale):
    return jax.random.normal(key, shape, jnp.float32) * scale


def setup_inputs(seed: int = 0, part: int = 0) -> dict:
    part_key = jax.random.fold_in(jax.random.key(seed), part)
    lat_keys = jax.random.split(part_key, 8)
    weight_keys = jax.random.split(jax.random.key(seed + 1), 20)
    group_ch = CHANNELS // NUM_GROUPS
    row_pos = (jnp.arange(LAT_ROWS, dtype=jnp.float32) + 0.5) / LAT_ROWS
    basis = jnp.cos(jnp.pi * row_pos[:, None] * jnp.arange(4, dtype=jnp.float32)[None, :])
    group_coef = draw_normal(lat_keys[0], (BATCH_SIZE, 4, NUM_GROUPS, 1), 1.0)
    chan_coef = draw_normal(lat_keys[1], (BATCH_SIZE, 4, NUM_GROUPS, group_ch), 0.5)
    mix_coef = (group_coef + chan_coef).reshape(BATCH_SIZE, 4, CHANNELS)
    row_mean = 0.7 * jnp.einsum('rk,bkc->brc', basis, mix_coef)
    scale_coef = draw_normal(lat_keys[2], (BATCH_SIZE, 4), 1.0)
    row_scale = jnp.exp(0.5 * jnp.einsum('rk,bk->br', basis, scale_coef))
    noise_vals = draw_normal(lat_keys[3], (BATCH_SIZE, LAT_ROWS, LAT_COLS, CHANNELS), 1.0)
    latent = row_mean[:, :, None, :] + row_scale[:, :, None, None] * noise_vals
    context = draw_normal(lat_keys[4], (BATCH_SIZE, 1, TEXT_DIM), 0.8) + draw_normal(lat_keys[5], (BATCH_SIZE, TEXT_LEN, TEXT_DIM), 1.0)
    chan_scale = CHANNELS ** -0.5
    out_boost = jnp.array([1.0, 1.0, 1.0, 2.0], jnp.float32).reshape(1, 4, 1, 1)
    arrays = {
        'latent': latent,
        'context': context,
        'gn_gain': 1.0 + draw_normal(weight_keys[0], (CHANNELS,), 0.3),
        'gn_bias': draw_normal(weight_keys[1], (CHANNELS,), 0.5),
        'w_in': draw_normal(weight_keys[2], (CHANNELS, CHANNELS), chan_scale),
        'b_in': draw_normal(weight_keys[3], (CHANNELS,), 0.5),
        'ln_gain': 1.0 + draw_normal(weight_keys[4], (NUM_LAYERS, 3, CHANNELS), 0.3),
        'ln_bias': draw_normal(weight_keys[5], (NUM_LAYERS, 3, CHANNELS), 0.3),
        'w_self': draw_normal(weight_keys[6], (NUM_LAYERS, 4, CHANNELS, CHANNELS), chan_scale) * out_boost,
        'b_self': draw_normal(weight_keys[7], (NUM_LAYERS, CHANNELS), 0.5),
        'w_cross_q': draw_normal(weight_keys[8], (NUM_LAYERS, CHANNELS, CHANNELS), chan_scale),
        'w_cross_kv': draw_normal(weight_keys[9], (NUM_LAYERS, 2, TEXT_DIM, CHANNELS), TEXT_DIM ** -0.5),
        'w_cross_o': draw_normal(weight_keys[10], (NUM_LAYERS, CHANNELS, CHANNELS), chan_scale),
        'b_cross': draw_normal(weight_keys[11], (NUM_LAYERS, CHANNELS), 0.5),
        'w_ff1': draw_normal(weight_keys[12], (NUM_LAYERS, CHANNELS, 2 * FF_DIM), chan_scale),
        'b_ff1': draw_normal(weight_keys[13], (NUM_LAYERS, 2 * FF_DIM), 0.5),
        'w_ff2': draw_normal(weight_keys[14], (NUM_LAYERS, FF_DIM, CHANNELS), FF_DIM ** -0.5),
        'b_ff2': draw_normal(weight_keys[15], (NUM_LAYERS, CHANNELS), 0.5),
        'w_out': draw_normal(weight_keys[16], (CHANNELS, CHANNELS), chan_scale),
        'b_out': draw_normal(weight_keys[17], (CHANNELS,), 0.5),
    }
    return {name: vals.astype(jnp.bfloat16) for name, vals in arrays.items()}


def layer_norm(hidden, gain, bias):
    vals = hidden.astype(jnp.float32)
    mean_val = jnp.mean(vals, axis=-1, keepdims=True)
    centered = vals - mean_val
    var_val = jnp.mean(centered * centered, axis=-1, keepdims=True)
    scaled = centered * lax.rsqrt(var_val + 1e-5)
    return (scaled * gain.astype(jnp.float32) + bias.astype(jnp.float32)).astype(jnp.bfloat16)


def project(act, weight):
    return jnp.dot(act, weight, preferred_element_type=jnp.float32)


def attend(query, keys, values):
    q_len = query.shape[0]
    k_len = keys.shape[0]
    q_heads = query.reshape(q_len, NUM_HEADS, HEAD_DIM).transpose(1, 0, 2)
    k_heads = keys.reshape(k_len, NUM_HEADS, HEAD_DIM).transpose(1, 0, 2)
    v_heads = values.reshape(k_len, NUM_HEADS, HEAD_DIM).transpose(1, 0, 2)

    def one_head(operands):
        q_one, k_one, v_one = operands
        scores = jnp.dot(q_one, k_one.T, preferred_element_type=jnp.float32) * (HEAD_DIM ** -0.5)
        attn_prob = jax.nn.softmax(scores, axis=-1).astype(jnp.bfloat16)
        return jnp.dot(attn_prob, v_one, preferred_element_type=jnp.float32).astype(jnp.bfloat16)

    head_out = lax.map(one_head, (q_heads, k_heads, v_heads))
    return head_out.transpose(1, 0, 2).reshape(q_len, NUM_HEADS * HEAD_DIM)


def reference(latent, context, gn_gain, gn_bias, w_in, b_in, ln_gain, ln_bias, w_self, b_self, w_cross_q, w_cross_kv, w_cross_o, b_cross, w_ff1, b_ff1, w_ff2, b_ff2, w_out, b_out):
    tokens = LAT_ROWS * LAT_COLS
    group_ch = CHANNELS // NUM_GROUPS

    def one_sample(operands):
        lat_one, ctx_one = operands
        lat_f32 = lat_one.astype(jnp.float32).reshape(tokens, NUM_GROUPS, group_ch)
        grp_mean = jnp.mean(lat_f32, axis=(0, 2), keepdims=True)
        centered = lat_f32 - grp_mean
        grp_var = jnp.mean(centered * centered, axis=(0, 2), keepdims=True)
        normed = (centered * lax.rsqrt(grp_var + 1e-6)).reshape(tokens, CHANNELS)
        normed = (normed * gn_gain.astype(jnp.float32) + gn_bias.astype(jnp.float32)).astype(jnp.bfloat16)
        hidden = (project(normed, w_in) + b_in.astype(jnp.float32)).astype(jnp.bfloat16)

        def block(hidden, layer_w):
            norm_gain, norm_bias, self_w, self_b, cross_q, cross_kv, cross_o, cross_b, ff_in, ff_in_bias, ff_outw, ff_out_bias = layer_w
            normed = layer_norm(hidden, norm_gain[0], norm_bias[0])
            query = project(normed, self_w[0]).astype(jnp.bfloat16)
            keys = project(normed, self_w[1]).astype(jnp.bfloat16)
            values = project(normed, self_w[2]).astype(jnp.bfloat16)
            attn_out = attend(query, keys, values)
            hidden = (hidden.astype(jnp.float32) + project(attn_out, self_w[3]) + self_b.astype(jnp.float32)).astype(jnp.bfloat16)
            normed = layer_norm(hidden, norm_gain[1], norm_bias[1])
            query = project(normed, cross_q).astype(jnp.bfloat16)
            keys = project(ctx_one, cross_kv[0]).astype(jnp.bfloat16)
            values = project(ctx_one, cross_kv[1]).astype(jnp.bfloat16)
            attn_out = attend(query, keys, values)
            hidden = (hidden.astype(jnp.float32) + project(attn_out, cross_o) + cross_b.astype(jnp.float32)).astype(jnp.bfloat16)
            normed = layer_norm(hidden, norm_gain[2], norm_bias[2])
            ff_proj = (project(normed, ff_in) + ff_in_bias.astype(jnp.float32)).astype(jnp.bfloat16)
            gated = (ff_proj[:, :FF_DIM].astype(jnp.float32) * jax.nn.gelu(ff_proj[:, FF_DIM:].astype(jnp.float32), approximate=False)).astype(jnp.bfloat16)
            hidden = (hidden.astype(jnp.float32) + project(gated, ff_outw) + ff_out_bias.astype(jnp.float32)).astype(jnp.bfloat16)
            return hidden, None

        layer_ws = (ln_gain, ln_bias, w_self, b_self, w_cross_q, w_cross_kv, w_cross_o, b_cross, w_ff1, b_ff1, w_ff2, b_ff2)
        hidden, scan_out = lax.scan(block, hidden, layer_ws)
        result = project(hidden, w_out) + b_out.astype(jnp.float32) + lat_one.reshape(tokens, CHANNELS).astype(jnp.float32)
        return result.astype(jnp.bfloat16).reshape(LAT_ROWS, LAT_COLS, CHANNELS)

    return lax.map(one_sample, (latent, context))
```

```python
import functools

import jax
import jax.numpy as jnp
from jax import lax
from jax.experimental import pallas as pl
from jax.experimental.pallas import tpu as pltpu
from jax.sharding import PartitionSpec as P

HEAD_DIM = 64
NUM_GROUPS = 32
LOG2E = 1.4426950408889634
VMEM_LIMIT = 60 * 1024 * 1024
F32 = jnp.float32
BF16 = jnp.bfloat16


def mm(lhs, rhs):
    return jnp.dot(lhs, rhs, preferred_element_type=F32)


def mm_nt(lhs, rhs):
    return lax.dot_general(lhs, rhs, (((1,), (1,)), ((), ())), preferred_element_type=F32)


def layer_norm(vals, gain_ref, bias_ref):
    mean_val = jnp.mean(vals, axis=-1, keepdims=True)
    centered = vals - mean_val
    var_val = jnp.mean(centered * centered, axis=-1, keepdims=True)
    scaled = centered * lax.rsqrt(var_val + 1e-5)
    return (scaled * gain_ref[...].astype(F32) + bias_ref[...].astype(F32)).astype(BF16)


def params(n_axes, flops, num_bytes):
    return dict(
        compiler_params=pltpu.CompilerParams(
            dimension_semantics=("arbitrary",) * n_axes, vmem_limit_bytes=VMEM_LIMIT
        ),
        cost_estimate=pl.CostEstimate(flops=int(flops), bytes_accessed=int(num_bytes), transcendentals=0),
    )


def in_kernel(x0, x1, x2, x3, gain_ref, bias_ref, sel_ref, selt_ref, w_ref, b_ref, o_ref, g_scr):
    blocks = (x0, x1, x2, x3)
    rows = x0.shape[0]
    group_ch = x0.shape[1] // NUM_GROUPS
    count = float(len(blocks) * rows * group_ch)

    def spread(col_sums):
        wide = jnp.broadcast_to(col_sums, (8, col_sums.shape[1]))
        grp = jnp.dot(wide, sel_ref[...], preferred_element_type=F32, precision=lax.Precision.HIGHEST)
        back = jnp.dot(grp, selt_ref[...], preferred_element_type=F32, precision=lax.Precision.HIGHEST)
        return back[0:1] / count

    total = sum(jnp.sum(r[...].astype(F32), axis=0, keepdims=True) for r in blocks)
    mean_val = spread(total)
    sq_total = jnp.zeros_like(total)
    for r in blocks:
        cent = r[...].astype(F32) - mean_val
        sq_total = sq_total + jnp.sum(cent * cent, axis=0, keepdims=True)
    inv_std = lax.rsqrt(spread(sq_total) + 1e-6)
    gain = gain_ref[...].astype(F32)
    bias = bias_ref[...].astype(F32)
    for n, r in enumerate(blocks):
        cent = r[...].astype(F32) - mean_val
        g_scr[n * rows : (n + 1) * rows, :] = (cent * inv_std * gain + bias).astype(BF16)
    o_ref[...] = (mm(g_scr[...], w_ref[...]) + b_ref[...].astype(F32)).astype(BF16)


def call_in(pieces, gn_gain, gn_bias, sel, selt, w_in, b_in):
    rows, ch = pieces[0].shape
    tokens = rows * len(pieces)
    full = lambda shape: pl.BlockSpec(shape, lambda i: (0,) * len(shape))
    return pl.pallas_call(
        in_kernel,
        grid=(1,),
        in_specs=[full((rows, ch))] * 4
        + [full((1, ch)), full((1, ch)), full(sel.shape), full(selt.shape), full((ch, ch)), full((1, ch))],
        out_specs=full((tokens, ch)),
        out_shape=jax.ShapeDtypeStruct((tokens, ch), BF16),
        scratch_shapes=[pltpu.VMEM((tokens, ch), BF16)],
        **params(1, 2 * tokens * ch * ch, 2 * ch * ch + 4 * tokens * ch),
        name="gn_in",
    )(*pieces, gn_gain, gn_bias, sel, selt, w_in, b_in)


def self_kernel(h_ref, gain_ref, bias_ref, wq_ref, wk_ref, wv_ref, wo_ref, bo_ref, o_ref, a_scr, acc_scr):
    step = pl.program_id(1)

    @pl.when(step == 0)
    def _():
        vals = h_ref[...].astype(F32)
        a_scr[...] = layer_norm(vals, gain_ref, bias_ref)
        acc_scr[...] = vals + bo_ref[...].astype(F32)

    act = a_scr[...]
    query = mm(act, wq_ref[...]).astype(BF16)
    keys = mm(act, wk_ref[...]).astype(BF16)
    values = mm(act, wv_ref[...]).astype(BF16)
    tokens = act.shape[0]
    low = lax.broadcasted_iota(jnp.int32, (1, 128), 1) < HEAD_DIM
    edge = (tokens // 128) * 128
    scale = HEAD_DIM**-0.5 * LOG2E
    outs = []
    for pair in range(query.shape[1] // 128):
        cols = slice(pair * 128, pair * 128 + 128)
        q_pair, k_pair, v_pair = query[:, cols], keys[:, cols], values[:, cols]
        zero = jnp.zeros_like(k_pair)
        k_stack = jnp.concatenate([jnp.where(low, k_pair, zero), jnp.where(low, zero, k_pair)], axis=0)
        v_stack = jnp.concatenate([jnp.where(low, v_pair, zero), jnp.where(low, zero, v_pair)], axis=0)
        scores = mm_nt(q_pair, k_stack)
        s_a = scores[:, :edge]
        s_mid = scores[:, edge : edge + 128]
        s_b = scores[:, edge + 128 :]
        neg = jnp.full_like(s_mid, -jnp.inf)
        max_a = jnp.maximum(
            jnp.max(s_a, axis=-1, keepdims=True), jnp.max(jnp.where(low, s_mid, neg), axis=-1, keepdims=True)
        )
        max_b = jnp.maximum(
            jnp.max(s_b, axis=-1, keepdims=True), jnp.max(jnp.where(low, neg, s_mid), axis=-1, keepdims=True)
        )
        e_a = jnp.exp2((s_a - max_a) * scale)
        e_b = jnp.exp2((s_b - max_b) * scale)
        e_mid = jnp.exp2((s_mid - jnp.where(low, max_a, max_b)) * scale)
        zmid = jnp.zeros_like(e_mid)
        sum_a = jnp.sum(e_a, axis=-1, keepdims=True) + jnp.sum(jnp.where(low, e_mid, zmid), axis=-1, keepdims=True)
        sum_b = jnp.sum(e_b, axis=-1, keepdims=True) + jnp.sum(jnp.where(low, zmid, e_mid), axis=-1, keepdims=True)
        inv_a = 1.0 / sum_a
        inv_b = 1.0 / sum_b
        prob = jnp.concatenate(
            [
                (e_a * inv_a).astype(BF16),
                (e_mid * jnp.where(low, inv_a, inv_b)).astype(BF16),
                (e_b * inv_b).astype(BF16),
            ],
            axis=1,
        )
        outs.append(mm(prob, v_stack).astype(BF16))
    acc_scr[...] += mm(jnp.concatenate(outs, axis=1), wo_ref[...])

    @pl.when(step == pl.num_programs(1) - 1)
    def _():
        o_ref[...] = acc_scr[...].astype(BF16)


def call_self(h, layer, ln_gain, ln_bias, w_self, b_self):
    samples, tokens, ch = h.shape
    width = 256
    steps = ch // width
    tok = pl.BlockSpec((None, tokens, ch), lambda s, i: (s, 0, 0))
    vec = lambda n: pl.BlockSpec((None, 1, ch), lambda s, i: (n, 0, 0))
    col = lambda j: pl.BlockSpec((None, None, ch, width), lambda s, i: (layer, j, 0, i))
    flops = samples * (2 * tokens * ch * ch * 4 + 4 * tokens * tokens * ch * 4)
    return pl.pallas_call(
        self_kernel,
        grid=(samples, steps),
        in_specs=[tok, vec(layer * 3), vec(layer * 3), col(0), col(1), col(2),
                  pl.BlockSpec((None, None, width, ch), lambda s, i: (layer, 3, i, 0)), vec(layer)],
        out_specs=tok,
        out_shape=jax.ShapeDtypeStruct(h.shape, BF16),
        scratch_shapes=[pltpu.VMEM((tokens, ch), BF16), pltpu.VMEM((tokens, ch), F32)],
        **params(2, flops, samples * (8 * ch * ch + 4 * tokens * ch)),
        name="self_attn",
    )(h, ln_gain, ln_bias, w_self, w_self, w_self, w_self, b_self)


def cross_kernel(text_len, h_ref, gain_ref, bias_ref, wq_ref, k_ref, v_ref, wo_ref, bo_ref, *rest):
    o_ref, a_scr, acc_scr = rest[-3:]
    step = pl.program_id(1)

    @pl.when(step == 0)
    def _():
        vals = h_ref[...].astype(F32)
        a_scr[...] = layer_norm(vals, gain_ref, bias_ref)
        acc_scr[...] = vals + bo_ref[...].astype(F32)

    query = mm(a_scr[...], wq_ref[...]).astype(BF16)
    low = lax.broadcasted_iota(jnp.int32, (1, 128), 1) < HEAD_DIM
    valid = lax.broadcasted_iota(jnp.int32, (1, 128), 1) < text_len
    scale = HEAD_DIM**-0.5 * LOG2E
    pad = jnp.zeros((128 - k_ref.shape[0], 128), BF16)
    outs = []
    for pair in range(query.shape[1] // 128):
        cols = slice(pair * 128, pair * 128 + 128)
        k_pair = jnp.concatenate([k_ref[:, cols], pad], axis=0)
        v_pair = jnp.concatenate([v_ref[:, cols], pad], axis=0)
        zero = jnp.zeros_like(k_pair)
        k_stack = jnp.concatenate([jnp.where(low, k_pair, zero), jnp.where(low, zero, k_pair)], axis=0)
        v_stack = jnp.concatenate([jnp.where(low, v_pair, zero), jnp.where(low, zero, v_pair)], axis=0)
        scores = mm_nt(query[:, cols], k_stack)
        probs = []
        for half in range(2):
            s_one = jnp.where(valid, scores[:, half * 128 : half * 128 + 128], -jnp.inf)
            e_one = jnp.exp2((s_one - jnp.max(s_one, axis=-1, keepdims=True)) * scale)
            inv = 1.0 / jnp.sum(e_one, axis=-1, keepdims=True)
            probs.append((e_one * inv).astype(BF16))
        outs.append(mm(jnp.concatenate(probs, axis=1), v_stack).astype(BF16))
    acc_scr[...] += mm(jnp.concatenate(outs, axis=1), wo_ref[...])

    @pl.when(step == pl.num_programs(1) - 1)
    def _():
        o_ref[...] = acc_scr[...].astype(BF16)


def call_cross(h, layer, text_len, k_text, v_text, first, total, buf, ln_gain, ln_bias, w_q, w_o, b_cross):
    samples, tokens, ch = h.shape
    width = 256
    steps = ch // width
    key_rows = k_text.shape[1]
    tok = pl.BlockSpec((None, tokens, ch), lambda s, i: (s, 0, 0))
    out = pl.BlockSpec((None, tokens, ch), lambda s, i: (s + first, 0, 0))
    vec = lambda n: pl.BlockSpec((None, 1, ch), lambda s, i: (n, 0, 0))
    txt = pl.BlockSpec((None, key_rows, width), lambda s, i: (s + first, 0, i))
    in_specs = [tok, vec(layer * 3 + 1), vec(layer * 3 + 1),
                pl.BlockSpec((None, ch, width), lambda s, i: (layer, 0, i)), txt, txt,
                pl.BlockSpec((None, width, ch), lambda s, i: (layer, i, 0)), vec(layer)]
    args = [h, ln_gain, ln_bias, w_q, k_text, v_text, w_o, b_cross]
    aliases = {}
    if buf is not None:
        in_specs.append(pl.BlockSpec(memory_space=pl.ANY))
        args.append(buf)
        aliases = {len(args) - 1: 0}
    flops = samples * (2 * tokens * ch * ch * 2 + 4 * tokens * 128 * ch)
    return pl.pallas_call(
        functools.partial(cross_kernel, text_len),
        grid=(samples, steps),
        in_specs=in_specs,
        out_specs=out,
        out_shape=jax.ShapeDtypeStruct((total, tokens, ch), BF16),
        scratch_shapes=[pltpu.VMEM((tokens, ch), BF16), pltpu.VMEM((tokens, ch), F32)],
        input_output_aliases=aliases,
        **params(2, flops, samples * (4 * ch * ch + 4 * tokens * ch)),
        name="cross_attn",
    )(*args)


def ff_kernel(chunks, tiles, h_ref, gain_ref, bias_ref, wp_ref, wq_ref, bp_ref, bq_ref, w2_ref, b2_ref, o_ref, a_scr, acc_scr, u_scr):
    step = pl.program_id(0)
    last = chunks * tiles
    rows = h_ref.shape[0]
    width = wp_ref.shape[1]

    @pl.when(step < chunks)
    def _():
        vals = h_ref[...].astype(F32)
        at = pl.ds(pl.multiple_of(step * rows, rows), rows)
        a_scr[at, :] = layer_norm(vals, gain_ref, bias_ref)
        acc_scr[at, :] = vals + b2_ref[...].astype(F32)

    def first_half():
        at = pl.ds(pl.multiple_of(lax.rem(step, chunks) * rows, rows), rows)
        act = a_scr[at, :]
        slot = lax.rem(step, 2)
        u_scr[slot, :, :width] = (mm(act, wp_ref[...]) + bp_ref[...].astype(F32)).astype(BF16)
        u_scr[slot, :, width:] = (mm(act, wq_ref[...]) + bq_ref[...].astype(F32)).astype(BF16)

    def second_half():
        at = pl.ds(pl.multiple_of(lax.rem(step - 1, chunks) * rows, rows), rows)
        slot = lax.rem(step - 1, 2)
        p_val = u_scr[slot, :, :width].astype(F32)
        q_val = u_scr[slot, :, width:].astype(F32)
        gate = 0.5 * q_val * (1.0 + lax.erf(q_val * (2.0**-0.5)))
        gated = (p_val * gate).astype(BF16)
        acc_scr[at, :] += mm(gated, w2_ref[...])

    @pl.when(step == 0)
    def _():
        first_half()

    @pl.when((step > 0) & (step < last))
    def _():
        second_half()
        first_half()

    @pl.when(step == last)
    def _():
        second_half()

    @pl.when(step > last - chunks)
    def _():
        at = pl.ds(pl.multiple_of(lax.rem(step - 1, chunks) * rows, rows), rows)
        o_ref[...] = acc_scr[at, :].astype(BF16)


def call_ff(h, layer, first, samples, ln_gain, ln_bias, w1, b1, w2, b2):
    tokens, ch = h.shape[1:]
    ff_dim = w2.shape[1]
    width = 512
    tiles = ff_dim // width
    chunks = samples
    last = chunks * tiles
    tile = lambda s: jnp.minimum(s // chunks, tiles - 1)
    lag_tile = lambda s: jnp.maximum(s - 1, 0) // chunks
    done = lambda s: jnp.where(s > last - chunks, lax.rem(jnp.maximum(s - 1, 0), chunks), 0)
    vec = lambda n, size: pl.BlockSpec((None, 1, size), lambda s: (n, 0, 0))
    flops = 6 * chunks * tokens * ch * ff_dim
    return pl.pallas_call(
        functools.partial(ff_kernel, chunks, tiles),
        grid=(last + 1,),
        in_specs=[
            pl.BlockSpec((None, tokens, ch), lambda s: (first + jnp.minimum(s, chunks - 1), 0, 0)),
            vec(layer * 3 + 2, ch),
            vec(layer * 3 + 2, ch),
            pl.BlockSpec((None, ch, width), lambda s: (layer, 0, tile(s))),
            pl.BlockSpec((None, ch, width), lambda s: (layer, 0, tiles + tile(s))),
            pl.BlockSpec((None, 1, width), lambda s: (layer, 0, tile(s))),
            pl.BlockSpec((None, 1, width), lambda s: (layer, 0, tiles + tile(s))),
            pl.BlockSpec((None, width, ch), lambda s: (layer, lag_tile(s), 0)),
            vec(layer, ch),
        ],
        out_specs=pl.BlockSpec((None, tokens, ch), lambda s: (done(s), 0, 0)),
        out_shape=jax.ShapeDtypeStruct((samples, tokens, ch), BF16),
        scratch_shapes=[
            pltpu.VMEM((chunks * tokens, ch), BF16),
            pltpu.VMEM((chunks * tokens, ch), F32),
            pltpu.VMEM((2, tokens, 2 * width), BF16),
        ],
        **params(1, flops, 6 * ch * ff_dim + 4 * chunks * tokens * ch),
        name="geglu_ff",
    )(h, ln_gain, ln_bias, w1, w1, b1, b1, w2, b2)


def out_kernel(me_ref, h0, h1, h2, h3, x_ref, w_ref, b_ref, *rest):
    y_ref = rest[-1]
    k = pl.program_id(0)
    for n, r in enumerate((h0, h1, h2, h3)):

        @pl.when(k == n)
        def _():
            y_ref[...] = (mm(r[...], w_ref[...]) + b_ref[...].astype(F32) + x_ref[...].astype(F32)).astype(BF16)


def call_out(me, slot, per_dev, pieces, x, w_out, b_out, buf):
    rows, ch = pieces[0].shape
    full = lambda shape: pl.BlockSpec(shape, lambda k, m: (0,) * len(shape))
    place = pl.BlockSpec((None, rows, ch), lambda k, m: (per_dev * jnp.bitwise_xor(m[0], k) + slot, 0, 0))
    in_specs = [full((rows, ch))] * 4 + [place, full((ch, ch)), full((1, ch))]
    args = [*pieces, x, w_out, b_out]
    aliases = {}
    if buf is not None:
        in_specs.append(pl.BlockSpec(memory_space=pl.ANY))
        args.append(buf)
        aliases = {len(args): 0}
    return pl.pallas_call(
        out_kernel,
        grid_spec=pltpu.PrefetchScalarGridSpec(
            num_scalar_prefetch=1, grid=(len(pieces),), in_specs=in_specs, out_specs=place
        ),
        out_shape=jax.ShapeDtypeStruct(x.shape, BF16),
        input_output_aliases=aliases,
        **params(1, 2 * len(pieces) * rows * ch * ch, 2 * ch * ch + 6 * len(pieces) * rows * ch),
        name="proj_out",
    )(me, *args)


def text_proj(ctx, w_kv):
    samples, length, dim = ctx.shape
    flat = ctx.reshape(samples * length, dim)
    return tuple(mm(flat, w_kv[j]).astype(BF16).reshape(samples, length, -1) for j in range(2))


def solution(mesh):
    n = mesh.shape["sp"]
    tok_spec = P("dp", "sp", None, None)
    ctx_spec = P("dp", None, None)
    replicated = P()

    def local_forward(latent, context, gn_gain, gn_bias, w_in, b_in, ln_gain, ln_bias, w_self, b_self, w_cross_q, w_cross_kv, w_cross_o, b_cross, w_ff1, b_ff1, w_ff2, b_ff2, w_out, b_out):
        batch, rows, columns, ch = latent.shape
        tokens = rows * columns
        layers = w_self.shape[0]
        per_dev = batch // n
        me = lax.axis_index("sp")
        x = latent.reshape(batch, tokens, ch)
        swap = lambda val, k: lax.ppermute(val, "sp", [(i, i ^ k) for i in range(n)])

        pieces = []
        for j in range(per_dev):
            take = lambda k: lax.dynamic_index_in_dim(x, per_dev * jnp.bitwise_xor(me, k) + j, 0, keepdims=False)
            pieces.append([take(0)] + [swap(take(k), k) for k in range(1, n)])

        text_len = context.shape[1]
        ctx = lax.dynamic_slice_in_dim(context, per_dev * me, per_dev, 0)
        ctx = jnp.pad(ctx, ((0, 0), (0, -text_len % 16), (0, 0)))
        text = [text_proj(ctx, w_cross_kv[layer]) for layer in range(layers)]

        group = jnp.arange(ch)[:, None] // (ch // NUM_GROUPS)
        sel = (group == jnp.arange(128)[None, :]).astype(F32)
        row = lambda val: val.reshape(-1, 1, ch)
        ln_gain, ln_bias = row(ln_gain), row(ln_bias)
        b_self, b_cross, b_ff2 = row(b_self), row(b_cross), row(b_ff2)
        b_ff1 = b_ff1[:, None, :]
        cross = lambda h, layer, first, buf: call_cross(
            h, layer, text_len, *text[layer], first, per_dev, buf, ln_gain, ln_bias, w_cross_q, w_cross_o, b_cross)

        h = None
        for j in range(per_dev):
            one = call_in(pieces[j], gn_gain[None], gn_bias[None], sel, sel.T, w_in, b_in[None])
            one = call_self(one[None], 0, ln_gain, ln_bias, w_self, b_self)
            h = cross(one, 0, j, h)
        for layer in range(1, layers):
            h = call_ff(h, layer - 1, 0, per_dev, ln_gain, ln_bias, w_ff1, b_ff1, w_ff2, b_ff2)
            h = call_self(h, layer, ln_gain, ln_bias, w_self, b_self)
            h = cross(h, layer, 0, None)
        groups = [(0, 2), (2, 1), (3, 1)] if per_dev == 4 else [(j, 1) for j in range(per_dev)]
        y = None
        me_arr = me.astype(jnp.int32).reshape(1)
        for first, count in groups:
            part = call_ff(h, layers - 1, first, count, ln_gain, ln_bias, w_ff1, b_ff1, w_ff2, b_ff2)
            for j in range(count):
                back = [part[j, k * tokens : (k + 1) * tokens] for k in range(n)]
                back = [back[0]] + [swap(back[k], k) for k in range(1, n)]
                y = call_out(me_arr, first + j, per_dev, back, x, w_out, b_out[None], y)
        return y.reshape(latent.shape)

    in_specs = (tok_spec, ctx_spec) + (replicated,) * 18
    return jax.shard_map(local_forward, mesh=mesh, in_specs=in_specs, out_specs=tok_spec, check_vma=False)
```

```python
import functools

import jax
import jax.numpy as jnp
from jax import lax
from jax.experimental import pallas as pl
from jax.experimental.pallas import tpu as pltpu
from jax.sharding import PartitionSpec as P

HEAD_DIM = 64
NUM_GROUPS = 32
LOG2E = 1.4426950408889634
VMEM_LIMIT = 60 * 1024 * 1024
F32 = jnp.float32
BF16 = jnp.bfloat16


def mm(lhs, rhs):
    return jnp.dot(lhs, rhs, preferred_element_type=F32)


def mm_nt(lhs, rhs):
    return lax.dot_general(lhs, rhs, (((1,), (1,)), ((), ())), preferred_element_type=F32)


def norm_rows(h_ref, gain, bias, a_ref, start, count, res_ref=None, res_bias=None, offset=0, part=16):
    for m in range(0, count, part):
        at = pl.multiple_of(start + m, part)
        vals = h_ref[pl.ds(at, part), :].astype(F32)
        mean_val = jnp.mean(vals, axis=-1, keepdims=True)
        centered = vals - mean_val
        var_val = jnp.mean(centered * centered, axis=-1, keepdims=True)
        scaled = centered * lax.rsqrt(var_val + 1e-5)
        dst = pl.ds(pl.multiple_of(offset + at, part), part)
        a_ref[dst, :] = (scaled * gain + bias).astype(BF16)
        if res_ref is not None:
            res_ref[dst, :] = vals + res_bias


def norm_all(h_ref, gain, bias, a_ref, res_ref=None, res_bias=None, offset=0):
    half = h_ref.shape[0] // 2

    def body(n, carry):
        norm_rows(h_ref, gain, bias, a_ref, n * half, half, res_ref, res_bias, offset)
        return carry

    lax.fori_loop(0, 2, body, 0)


def params(n_axes, flops, num_bytes):
    return dict(
        compiler_params=pltpu.CompilerParams(
            dimension_semantics=("arbitrary",) * n_axes, vmem_limit_bytes=VMEM_LIMIT
        ),
        cost_estimate=pl.CostEstimate(flops=int(flops), bytes_accessed=int(num_bytes), transcendentals=0),
    )


def in_kernel(x0, x1, x2, x3, gain_ref, bias_ref, w_ref, b_ref, o_ref, g_scr):
    blocks = (x0, x1, x2, x3)
    rows, ch = x0.shape
    group_ch = ch // NUM_GROUPS
    count = float(len(blocks) * rows * group_ch)
    chan = lax.broadcasted_iota(jnp.int32, (ch, 128), 0)
    low = lax.broadcasted_iota(jnp.int32, (ch, 128), 1) * group_ch
    sel = ((chan >= low) & (chan < low + group_ch)).astype(BF16)

    def parts(val):
        hi = val.astype(BF16)
        rest = val - hi.astype(F32)
        mid = rest.astype(BF16)
        lo = (rest - mid.astype(F32)).astype(BF16)
        tail = jnp.zeros((13, val.shape[1]), BF16)
        return jnp.concatenate([hi, mid, lo, tail], axis=0)

    def spread(col_sums):
        grp = jnp.sum(mm(parts(col_sums), sel), axis=0, keepdims=True) / count
        return jnp.sum(mm_nt(parts(grp), sel), axis=0, keepdims=True)

    def col_sum(fn):
        part = 16
        total = jnp.zeros((part, ch), F32)
        for r in blocks:
            for m in range(rows // part):
                total = total + fn(r[m * part : (m + 1) * part, :].astype(F32))
        return jnp.sum(total, axis=0, keepdims=True)

    mean_val = spread(col_sum(lambda val: val))
    inv_std = lax.rsqrt(spread(col_sum(lambda val: (val - mean_val) * (val - mean_val))) + 1e-6)
    gain = gain_ref[...].astype(F32)
    bias = bias_ref[...].astype(F32)
    for n, r in enumerate(blocks):
        for m in range(0, rows, 16):
            vals = r[m : m + 16, :].astype(F32)
            g_scr[n * rows + m : n * rows + m + 16, :] = ((vals - mean_val) * inv_std * gain + bias).astype(BF16)
    o_ref[...] = (mm(g_scr[...], w_ref[...]) + b_ref[...].astype(F32)).astype(BF16)


def call_in(pieces, gn_gain, gn_bias, w_in, b_in):
    samples, rows, ch = pieces[0].shape
    tokens = rows * len(pieces)
    full = lambda shape: pl.BlockSpec(shape, lambda i: (0,) * len(shape))
    return pl.pallas_call(
        in_kernel,
        grid=(samples,),
        in_specs=[pl.BlockSpec((None, rows, ch), lambda i: (i, 0, 0))] * 4
        + [full((1, ch)), full((1, ch)), full((ch, ch)), full((1, ch))],
        out_specs=pl.BlockSpec((None, tokens, ch), lambda i: (i, 0, 0)),
        out_shape=jax.ShapeDtypeStruct((samples, tokens, ch), BF16),
        scratch_shapes=[pltpu.VMEM((tokens, ch), BF16)],
        **params(1, samples * 2 * tokens * ch * ch, 2 * ch * ch + samples * 4 * tokens * ch),
        name="gn_in",
    )(*pieces, gn_gain, gn_bias, w_in, b_in)


def split_heads(val, low):
    zero = jnp.zeros_like(val)
    return jnp.concatenate([jnp.where(low, val, zero), jnp.where(low, zero, val)], axis=0)


def pair_softmax(scores, low, valid=None):
    scale = HEAD_DIM**-0.5 * LOG2E
    tiles = [scores[:, n : n + 128] for n in range(0, scores.shape[1], 128)]
    half, shared = divmod(len(tiles), 2)
    if valid is not None:
        tiles = [jnp.where(valid, tile, -jnp.inf) for tile in tiles]

    def reduce(vals, op, fill, lanes):
        first, second = vals[:half], vals[half + shared :]
        if shared:
            pad = jnp.full_like(vals[half], fill)
            first = first + [jnp.where(low, vals[half], pad)]
            second = second + [jnp.where(low, pad, vals[half])]
        return [lanes(functools.reduce(op, part), axis=-1, keepdims=True) for part in (first, second)]

    def pick(pair, n):
        return pair[0] if n < half else jnp.where(low, *pair) if n < half + shared else pair[1]

    peaks = reduce(tiles, jnp.maximum, -jnp.inf, jnp.max)
    exps = [jnp.exp2((tile - pick(peaks, n)) * scale) for n, tile in enumerate(tiles)]
    invs = [1.0 / val for val in reduce(exps, jnp.add, 0.0, jnp.sum)]
    return jnp.concatenate([(val * pick(invs, n)).astype(BF16) for n, val in enumerate(exps)], axis=1)


def attn_kernel(layer, norm, samples, groups, text_len, h_ref, old_ref, gain_ref, bias_ref, *refs):
    o_ref, a_scr, b_scr, acc_scr, cur_scr, nxt_scr = refs[-6:]
    if text_len:
        wq_ref, k_ref, v_ref, wo_ref, bo_ref = refs[:5]
    else:
        wq_ref, wk_ref, wv_ref, wo_ref, bo_ref = refs[:5]
    step = pl.program_id(0)
    last = samples * groups
    width = wq_ref.shape[1]
    tokens = h_ref.shape[0]
    half = tokens // 2
    halves = [slice(0, half), slice(half, tokens)]
    pairs = range(width // 128)

    group = lax.rem(step, groups)
    chunk = tokens // (groups - 1)
    gain = gain_ref[layer, norm : norm + 1].astype(F32)
    bias = bias_ref[layer, norm : norm + 1].astype(F32)

    @pl.when((group == 0) & (step > 0) & (step < last))
    def _():
        a_scr[...] = b_scr[...]

    def project(dst, n, ref):
        for rows in halves:
            dst[rows, n * width : (n + 1) * width] = mm(a_scr[rows, :], ref[...]).astype(BF16)

    def project_all(dst):
        for n, ref in enumerate((wq_ref,) if text_len else (wq_ref, wk_ref, wv_ref)):
            project(dst, n, ref)

    def attend(dst):
        lane = lax.broadcasted_iota(jnp.int32, (1, 128), 1)
        low = lane < HEAD_DIM
        at = lambda n, pair: slice(n * width + pair * 128, n * width + pair * 128 + 128)

        def text(ref, pair):
            pad = jnp.zeros((128 - ref.shape[0], 128), BF16)
            return jnp.concatenate([ref[:, at(0, pair)], pad], axis=0)

        def weigh(pair):
            keys = split_heads(text(k_ref, pair) if text_len else cur_scr[:, at(1, pair)], low)
            return [mm_nt(cur_scr[rows, at(0, pair)], keys) for rows in halves]

        def mix(pair, scores):
            vals = split_heads(text(v_ref, pair) if text_len else cur_scr[:, at(2, pair)], low)
            probs = [pair_softmax(val, low, lane < text_len if text_len else None) for val in scores]
            return jnp.concatenate([mm(prob, vals).astype(BF16) for prob in probs], axis=0)

        if text_len:
            scores = [weigh(pair) for pair in pairs]
            if dst is not None:
                project(dst, 0, wq_ref)
            outs = [mix(pair, scores[pair]) for pair in pairs]
        else:
            first = weigh(0)
            if dst is not None:
                project(dst, 0, wq_ref)
                project(dst, 1, wk_ref)
            second = weigh(1)
            outs = [mix(0, first)]
            if dst is not None:
                project(dst, 2, wv_ref)
            outs.append(mix(1, second))
        acc_scr[...] += mm(jnp.concatenate(outs, axis=1), wo_ref[...])

    @pl.when(step == 0)
    def _():
        norm_all(h_ref, gain, bias, a_scr)
        acc_scr[...] = jnp.zeros_like(acc_scr)
        project_all(cur_scr)

    @pl.when((step > 0) & (step < last))
    def _():
        if samples > 1:
            norm_rows(h_ref, gain, bias, b_scr, jnp.maximum(group - 1, 0) * chunk, chunk)
        attend(nxt_scr)
        cur_scr[...] = nxt_scr[...]

    @pl.when(step == last)
    def _():
        attend(None)

    @pl.when((group == 0) & (step > 0))
    def _():
        o_ref[...] = (acc_scr[...] + old_ref[...].astype(F32) + bo_ref[layer : layer + 1].astype(F32)).astype(BF16)
        acc_scr[...] = jnp.zeros_like(acc_scr)


def call_attn(h, layer, norm, first, total, buf, text_len, ln_gain, ln_bias, mids, mid_specs, w_o, wo_lead, b_o, width, parts, flops, name):
    samples, tokens, ch = h.shape
    groups = ch // width
    last = samples * groups
    now = lambda t: jnp.minimum(t, last - 1)
    lag = lambda t: jnp.maximum(t - 1, 0)
    full = lambda shape: pl.BlockSpec(shape, lambda t: (0,) * len(shape))
    lead = (None,) * len(wo_lead)
    in_specs = [
        pl.BlockSpec((None, tokens, ch), lambda t: (jnp.where(t == 0, 0, jnp.minimum(t // groups + 1, samples - 1)), 0, 0)),
        pl.BlockSpec((None, tokens, ch), lambda t: (lag(t) // groups, 0, 0)),
        full(ln_gain.shape), full(ln_bias.shape),
        *mid_specs(now, lag, groups),
        pl.BlockSpec((*lead, width, ch), lambda t: (*wo_lead, lax.rem(lag(t), groups), 0)), full(b_o.shape),
    ]
    args = [h, h, ln_gain, ln_bias, *mids, w_o, b_o]
    aliases = {}
    if buf is not None:
        in_specs.append(pl.BlockSpec(memory_space=pl.ANY))
        args.append(buf)
        aliases = {len(args) - 1: 0}
    return pl.pallas_call(
        functools.partial(attn_kernel, layer, norm, samples, groups, text_len),
        grid=(last + 1,),
        in_specs=in_specs,
        out_specs=pl.BlockSpec((None, tokens, ch), lambda t: (first + lag(t) // groups, 0, 0)),
        out_shape=jax.ShapeDtypeStruct((total, tokens, ch), BF16),
        scratch_shapes=[
            pltpu.VMEM((tokens, ch), BF16),
            pltpu.VMEM((tokens, ch), BF16),
            pltpu.VMEM((tokens, ch), F32),
            pltpu.VMEM((tokens, parts * width), BF16),
            pltpu.VMEM((tokens, parts * width), BF16),
        ],
        input_output_aliases=aliases,
        **params(1, flops, samples * (2 * (parts + 1) * ch * ch + 4 * tokens * ch)),
        name=name,
    )(*args)


def call_self(h, layer, first, total, buf, ln_gain, ln_bias, w_self, b_self):
    samples, tokens, ch = h.shape
    width = 256
    flops = samples * (2 * tokens * ch * ch * 4 + 4 * tokens * tokens * ch * 4)

    def mid_specs(now, lag, groups):
        col = lambda j: pl.BlockSpec((None, None, ch, width), lambda t: (layer, j, 0, lax.rem(now(t), groups)))
        return [col(0), col(1), col(2)]

    return call_attn(h, layer, 0, first, total, buf, 0, ln_gain, ln_bias, [w_self] * 3, mid_specs, w_self, (layer, 3),
                     b_self, width, 3, flops, "self_attn")


def call_cross(h, layer, text_len, k_text, v_text, ln_gain, ln_bias, w_q, w_o, b_cross):
    samples, tokens, ch = h.shape
    width = 256
    key_rows = k_text.shape[1]
    flops = samples * (2 * tokens * ch * ch * 2 + 4 * tokens * 128 * ch)

    def mid_specs(now, lag, groups):
        txt = pl.BlockSpec((None, key_rows, width), lambda t: (lag(t) // groups, 0, lax.rem(lag(t), groups)))
        return [pl.BlockSpec((None, ch, width), lambda t: (layer, 0, lax.rem(now(t), groups))), txt, txt]

    return call_attn(h, layer, 1, 0, samples, None, text_len, ln_gain, ln_bias, [w_q, k_text, v_text], mid_specs, w_o,
                     (layer,), b_cross, width, 1, flops, "cross_attn")


def ff_kernel(layer, chunks, tiles, h_ref, gain_ref, bias_ref, wp_ref, wq_ref, bp_ref, bq_ref, w2_ref, b2_ref, o_ref, a_scr, acc_scr, *z_scrs):
    step = pl.program_id(0)
    last = chunks * tiles
    rows = h_ref.shape[0]

    @pl.when(step < chunks)
    def _():
        norm_all(
            h_ref, gain_ref[layer, 2:3].astype(F32), bias_ref[layer, 2:3].astype(F32), a_scr,
            acc_scr, b2_ref[layer : layer + 1].astype(F32), offset=step * rows,
        )

    def first_half(dst):
        at = pl.ds(pl.multiple_of(lax.rem(step, chunks) * rows, rows), rows)
        act = a_scr[at, :]
        for n in range(0, dst.shape[1], 256):
            cols = slice(n, n + 256)
            p_val = (mm(act, wp_ref[:, cols]) + bp_ref[layer : layer + 1, cols].astype(F32)).astype(BF16).astype(F32)
            q_val = (mm(act, wq_ref[:, cols]) + bq_ref[layer : layer + 1, cols].astype(F32)).astype(BF16).astype(F32)
            gate = 0.5 * q_val * (1.0 + lax.erf(q_val * (2.0**-0.5)))
            dst[:, cols] = (p_val * gate).astype(BF16)

    def second_half(src):
        at = pl.ds(pl.multiple_of(lax.rem(step - 1, chunks) * rows, rows), rows)
        acc_scr[at, :] += mm(src[...], w2_ref[...])

    @pl.when(step == 0)
    def _():
        first_half(z_scrs[0])

    for parity in range(2):

        @pl.when((step > 0) & (step < last) & (lax.rem(step, 2) == parity))
        def _():
            first_half(z_scrs[parity])
            second_half(z_scrs[1 - parity])

    @pl.when(step == last)
    def _():
        second_half(z_scrs[(last - 1) % 2])

    @pl.when(step > last - chunks)
    def _():
        at = pl.ds(pl.multiple_of(lax.rem(step - 1, chunks) * rows, rows), rows)
        o_ref[...] = acc_scr[at, :].astype(BF16)


def call_ff(h, layer, first, samples, ln_gain, ln_bias, w1, b1, w2, b2):
    tokens, ch = h.shape[1:]
    ff_dim = w2.shape[1]
    width = 512
    tiles = ff_dim // width
    chunks = samples
    last = chunks * tiles
    tile = lambda s: jnp.minimum(s // chunks, tiles - 1)
    lag_tile = lambda s: jnp.maximum(s - 1, 0) // chunks
    done = lambda s: jnp.where(s > last - chunks, lax.rem(jnp.maximum(s - 1, 0), chunks), 0)
    full = lambda shape: pl.BlockSpec(shape, lambda s: (0,) * len(shape))
    flops = 6 * chunks * tokens * ch * ff_dim
    return pl.pallas_call(
        functools.partial(ff_kernel, layer, chunks, tiles),
        grid=(last + 1,),
        in_specs=[
            pl.BlockSpec((None, tokens, ch), lambda s: (first + jnp.minimum(s, chunks - 1), 0, 0)),
            full(ln_gain.shape),
            full(ln_bias.shape),
            pl.BlockSpec((None, ch, width), lambda s: (layer, 0, tile(s))),
            pl.BlockSpec((None, ch, width), lambda s: (layer, 0, tiles + tile(s))),
            pl.BlockSpec((b1.shape[0], width), lambda s: (0, tile(s))),
            pl.BlockSpec((b1.shape[0], width), lambda s: (0, tiles + tile(s))),
            pl.BlockSpec((None, width, ch), lambda s: (layer, lag_tile(s), 0)),
            full(b2.shape),
        ],
        out_specs=pl.BlockSpec((None, tokens, ch), lambda s: (done(s), 0, 0)),
        out_shape=jax.ShapeDtypeStruct((samples, tokens, ch), BF16),
        scratch_shapes=[
            pltpu.VMEM((chunks * tokens, ch), BF16),
            pltpu.VMEM((chunks * tokens, ch), F32),
            pltpu.VMEM((tokens, width), BF16),
            pltpu.VMEM((tokens, width), BF16),
        ],
        **params(1, flops, 6 * ch * ff_dim + 4 * chunks * tokens * ch),
        name="geglu_ff",
    )(h, ln_gain, ln_bias, w1, w1, b1, b1, w2, b2)


def out_kernel(me_ref, h0, h1, h2, h3, x_ref, w_ref, b_ref, *rest):
    y_ref, p_scr, h_scr = rest[-3:]
    k = pl.program_id(1)
    rows = h0.shape[0]

    @pl.when(k == 0)
    def _():
        for n, r in enumerate((h0, h1, h2, h3)):
            h_scr[n * rows : (n + 1) * rows, :] = r[...]
        p_scr[...] = mm(h_scr[...], w_ref[...]) + b_ref[...].astype(F32)

    at = pl.ds(pl.multiple_of(k * rows, rows), rows)
    y_ref[...] = (p_scr[at, :] + x_ref[...].astype(F32)).astype(BF16)


def call_out(me, first, per_dev, pieces, x, w_out, b_out, buf):
    samples, rows, ch = pieces[0].shape
    n = len(pieces)
    full = lambda shape: pl.BlockSpec(shape, lambda s, k, m: (0,) * len(shape))
    place = pl.BlockSpec((None, rows, ch), lambda s, k, m: (per_dev * jnp.bitwise_xor(m[0], k) + first + s, 0, 0))
    in_specs = [pl.BlockSpec((None, rows, ch), lambda s, k, m: (s, 0, 0))] * n + [place, full((ch, ch)), full((1, ch))]
    args = [*pieces, x, w_out, b_out]
    aliases = {}
    if buf is not None:
        in_specs.append(pl.BlockSpec(memory_space=pl.ANY))
        args.append(buf)
        aliases = {len(args): 0}
    return pl.pallas_call(
        out_kernel,
        grid_spec=pltpu.PrefetchScalarGridSpec(
            num_scalar_prefetch=1, grid=(samples, n), in_specs=in_specs, out_specs=place,
            scratch_shapes=[pltpu.VMEM((n * rows, ch), F32), pltpu.VMEM((n * rows, ch), BF16)],
        ),
        out_shape=jax.ShapeDtypeStruct(x.shape, BF16),
        input_output_aliases=aliases,
        **params(2, samples * 2 * n * rows * ch * ch, 2 * ch * ch + samples * 6 * n * rows * ch),
        name="proj_out",
    )(me, *args)


def text_proj(ctx, w_kv):
    samples, length, dim = ctx.shape
    flat = ctx.reshape(samples * length, dim)
    return tuple(mm(flat, w_kv[j]).astype(BF16).reshape(samples, length, -1) for j in range(2))


def solution(mesh):
    n = mesh.shape["sp"]
    tok_spec = P("dp", "sp", None, None)
    ctx_spec = P("dp", None, None)
    replicated = P()

    def local_forward(latent, context, gn_gain, gn_bias, w_in, b_in, ln_gain, ln_bias, w_self, b_self, w_cross_q, w_cross_kv, w_cross_o, b_cross, w_ff1, b_ff1, w_ff2, b_ff2, w_out, b_out):
        batch, rows, columns, ch = latent.shape
        tokens = rows * columns
        layers = w_self.shape[0]
        per_dev = batch // n
        me = lax.axis_index("sp")
        x = latent.reshape(batch, tokens, ch)
        swap = lambda val, k: lax.ppermute(val, "sp", [(i, i ^ k) for i in range(n)])

        pieces = []
        for first in range(0, per_dev, 2):
            take = lambda k: lax.dynamic_slice_in_dim(x, per_dev * jnp.bitwise_xor(me, k) + first, 2, 0)
            pieces.append([take(0)] + [swap(take(k), k) for k in range(1, n)])

        text_len = context.shape[1]
        ctx = lax.dynamic_slice_in_dim(context, per_dev * me, per_dev, 0)
        ctx = jnp.pad(ctx, ((0, 0), (0, -text_len % 16), (0, 0)))
        text = [text_proj(ctx, w_cross_kv[layer]) for layer in range(layers)]

        h = None
        for g, blocks in enumerate(pieces):
            part = call_in(blocks, gn_gain[None], gn_bias[None], w_in, b_in[None])
            h = call_self(part, 0, 2 * g, per_dev, h, ln_gain, ln_bias, w_self, b_self)
        for layer in range(layers):
            if layer:
                h = call_self(h, layer, 0, per_dev, None, ln_gain, ln_bias, w_self, b_self)
            h = call_cross(h, layer, text_len, *text[layer], ln_gain, ln_bias, w_cross_q, w_cross_o, b_cross)
            if layer < layers - 1:
                h = call_ff(h, layer, 0, per_dev, ln_gain, ln_bias, w_ff1, b_ff1, w_ff2, b_ff2)
        y = None
        me_arr = me.astype(jnp.int32).reshape(1)
        for first, count in ((0, 2), (2, 1), (3, 1)):
            part = call_ff(h, layers - 1, first, count, ln_gain, ln_bias, w_ff1, b_ff1, w_ff2, b_ff2)
            h, part = lax.optimization_barrier((h, part))
            back = [part[:, k * tokens : (k + 1) * tokens] for k in range(n)]
            back = [back[0]] + [swap(back[k], k) for k in range(1, n)]
            y = call_out(me_arr, first, per_dev, back, x, w_out, b_out[None], y)
        return y.reshape(latent.shape)

    in_specs = (tok_spec, ctx_spec) + (replicated,) * 18
    return jax.shard_map(local_forward, mesh=mesh, in_specs=in_specs, out_specs=tok_spec, check_vma=False)
```

```python
import functools

import jax
import jax.numpy as jnp
from jax import lax
from jax.experimental import pallas as pl
from jax.experimental.pallas import tpu as pltpu
from jax.sharding import PartitionSpec as P


HEAD_DIM = 64
NUM_GROUPS = 32
LOG2E = 1.4426950408889634
VMEM_LIMIT = 60 * 1024 * 1024
F32 = jnp.float32
BF16 = jnp.bfloat16


def mm(lhs, rhs):
    return jnp.dot(lhs, rhs, preferred_element_type=F32)


def mm_nt(lhs, rhs):
    return lax.dot_general(lhs, rhs, (((1,), (1,)), ((), ())), preferred_element_type=F32)


def norm_rows(h_ref, gain, bias, a_ref, start, count, res_ref=None, res_bias=None, offset=0, part=16):
    for m in range(0, count, part):
        at = pl.multiple_of(start + m, part)
        vals = h_ref[pl.ds(at, part), :].astype(F32)
        mean_val = jnp.mean(vals, axis=-1, keepdims=True)
        centered = vals - mean_val
        var_val = jnp.mean(centered * centered, axis=-1, keepdims=True)
        scaled = centered * lax.rsqrt(var_val + 1e-5)
        dst = pl.ds(pl.multiple_of(offset + at, part), part)
        a_ref[dst, :] = (scaled * gain + bias).astype(BF16)
        if res_ref is not None:
            res_ref[dst, :] = vals + res_bias


def norm_all(h_ref, gain, bias, a_ref, res_ref=None, res_bias=None, offset=0):
    half = h_ref.shape[0] // 2

    def body(n, carry):
        norm_rows(h_ref, gain, bias, a_ref, n * half, half, res_ref, res_bias, offset)
        return carry

    lax.fori_loop(0, 2, body, 0)


def params(n_axes, flops, num_bytes):
    return dict(
        compiler_params=pltpu.CompilerParams(
            dimension_semantics=("arbitrary",) * n_axes, vmem_limit_bytes=VMEM_LIMIT
        ),
        cost_estimate=pl.CostEstimate(flops=int(flops), bytes_accessed=int(num_bytes), transcendentals=0),
    )


def in_kernel(x0, x1, x2, x3, gain_ref, bias_ref, w_ref, b_ref, o_ref, g_scr):
    blocks = (x0, x1, x2, x3)
    rows, ch = x0.shape
    group_ch = ch // NUM_GROUPS
    count = float(len(blocks) * rows * group_ch)
    chan = lax.broadcasted_iota(jnp.int32, (ch, 128), 0)
    low = lax.broadcasted_iota(jnp.int32, (ch, 128), 1) * group_ch
    sel = ((chan >= low) & (chan < low + group_ch)).astype(BF16)

    def parts(val):
        hi = val.astype(BF16)
        rest = val - hi.astype(F32)
        mid = rest.astype(BF16)
        lo = (rest - mid.astype(F32)).astype(BF16)
        tail = jnp.zeros((13, val.shape[1]), BF16)
        return jnp.concatenate([hi, mid, lo, tail], axis=0)

    def spread(col_sums):
        grp = jnp.sum(mm(parts(col_sums), sel), axis=0, keepdims=True) / count
        return jnp.sum(mm_nt(parts(grp), sel), axis=0, keepdims=True)

    def col_sum(fn):
        part = 16
        total = jnp.zeros((part, ch), F32)
        for r in blocks:
            for m in range(rows // part):
                total = total + fn(r[m * part : (m + 1) * part, :].astype(F32))
        return jnp.sum(total, axis=0, keepdims=True)

    mean_val = spread(col_sum(lambda val: val))
    inv_std = lax.rsqrt(spread(col_sum(lambda val: (val - mean_val) * (val - mean_val))) + 1e-6)
    gain = gain_ref[...].astype(F32)
    bias = bias_ref[...].astype(F32)
    for n, r in enumerate(blocks):
        for m in range(0, rows, 16):
            vals = r[m : m + 16, :].astype(F32)
            g_scr[n * rows + m : n * rows + m + 16, :] = ((vals - mean_val) * inv_std * gain + bias).astype(BF16)
    o_ref[...] = (mm(g_scr[...], w_ref[...]) + b_ref[...].astype(F32)).astype(BF16)


def call_in(pieces, gn_gain, gn_bias, w_in, b_in):
    samples, rows, ch = pieces[0].shape
    tokens = rows * len(pieces)
    full = lambda shape: pl.BlockSpec(shape, lambda i: (0,) * len(shape))
    return pl.pallas_call(
        in_kernel,
        grid=(samples,),
        in_specs=[pl.BlockSpec((None, rows, ch), lambda i: (i, 0, 0))] * 4
        + [full((1, ch)), full((1, ch)), full((ch, ch)), full((1, ch))],
        out_specs=pl.BlockSpec((None, tokens, ch), lambda i: (i, 0, 0)),
        out_shape=jax.ShapeDtypeStruct((samples, tokens, ch), BF16),
        scratch_shapes=[pltpu.VMEM((tokens, ch), BF16)],
        **params(1, samples * 2 * tokens * ch * ch, 2 * ch * ch + samples * 4 * tokens * ch),
        name="gn_in",
    )(*pieces, gn_gain, gn_bias, w_in, b_in)


def split_heads(val, low):
    zero = jnp.zeros_like(val)
    return jnp.concatenate([jnp.where(low, val, zero), jnp.where(low, zero, val)], axis=0)


def pair_softmax(scores, low, valid=None):
    scale = HEAD_DIM**-0.5 * LOG2E
    tiles = [scores[:, n : n + 128] for n in range(0, scores.shape[1], 128)]
    half, shared = divmod(len(tiles), 2)
    if valid is not None:
        tiles = [jnp.where(valid, tile, -jnp.inf) for tile in tiles]

    def reduce(vals, op, fill, lanes):
        first, second = vals[:half], vals[half + shared :]
        if shared:
            pad = jnp.full_like(vals[half], fill)
            first = first + [jnp.where(low, vals[half], pad)]
            second = second + [jnp.where(low, pad, vals[half])]
        return [lanes(functools.reduce(op, part), axis=-1, keepdims=True) for part in (first, second)]

    def pick(pair, n):
        return pair[0] if n < half else jnp.where(low, *pair) if n < half + shared else pair[1]

    peaks = reduce(tiles, jnp.maximum, -jnp.inf, jnp.max)
    exps = [jnp.exp2((tile - pick(peaks, n)) * scale) for n, tile in enumerate(tiles)]
    invs = [1.0 / val for val in reduce(exps, jnp.add, 0.0, jnp.sum)]
    return jnp.concatenate([(val * pick(invs, n)).astype(BF16) for n, val in enumerate(exps)], axis=1)


def attn_kernel(layer, norm, samples, groups, text_len, h_ref, old_ref, gain_ref, bias_ref, *refs):
    o_ref, a_scr, b_scr, acc_scr, cur_scr, nxt_scr = refs[-6:]
    if text_len:
        wq_ref, k_ref, v_ref, wo_ref, bo_ref = refs[:5]
    else:
        wq_ref, wk_ref, wv_ref, wo_ref, bo_ref = refs[:5]
    group = pl.program_id(1)
    step = pl.program_id(0) * groups + group
    last = samples * groups
    width = wq_ref.shape[1]
    tokens = h_ref.shape[0]
    half = tokens // 2
    halves = [slice(0, half), slice(half, tokens)]
    pairs = range(width // 128)

    chunk = tokens // (groups - 1)
    gain = gain_ref[layer, norm : norm + 1].astype(F32)
    bias = bias_ref[layer, norm : norm + 1].astype(F32)

    @pl.when((group == 0) & (step > 0) & (step < last))
    def _():
        a_scr[...] = b_scr[...]

    def project(dst, n, ref):
        for rows in halves:
            dst[rows, n * width : (n + 1) * width] = mm(a_scr[rows, :], ref[...]).astype(BF16)

    def project_all(dst):
        for n, ref in enumerate((wq_ref,) if text_len else (wq_ref, wk_ref, wv_ref)):
            project(dst, n, ref)

    def attend(dst):
        lane = lax.broadcasted_iota(jnp.int32, (1, 128), 1)
        low = lane < HEAD_DIM
        at = lambda n, pair: slice(n * width + pair * 128, n * width + pair * 128 + 128)

        def text(ref, pair):
            pad = jnp.zeros((128 - ref.shape[0], 128), BF16)
            return jnp.concatenate([ref[:, at(0, pair)], pad], axis=0)

        def weigh(pair):
            keys = split_heads(text(k_ref, pair) if text_len else cur_scr[:, at(1, pair)], low)
            return [mm_nt(cur_scr[rows, at(0, pair)], keys) for rows in halves]

        def mix(pair, scores):
            vals = split_heads(text(v_ref, pair) if text_len else cur_scr[:, at(2, pair)], low)
            probs = [pair_softmax(val, low, lane < text_len if text_len else None) for val in scores]
            return jnp.concatenate([mm(prob, vals).astype(BF16) for prob in probs], axis=0)

        if text_len:
            scores = [weigh(pair) for pair in pairs]
            if dst is not None:
                project(dst, 0, wq_ref)
            outs = [mix(pair, scores[pair]) for pair in pairs]
        else:
            first = weigh(0)
            if dst is not None:
                project(dst, 0, wq_ref)
                project(dst, 1, wk_ref)
            second = weigh(1)
            outs = [mix(0, first)]
            if dst is not None:
                project(dst, 2, wv_ref)
            outs.append(mix(1, second))
        acc_scr[...] += mm(jnp.concatenate(outs, axis=1), wo_ref[...])

    @pl.when(step == 0)
    def _():
        norm_all(h_ref, gain, bias, a_scr)
        acc_scr[...] = jnp.zeros_like(acc_scr)
        project_all(cur_scr)

    @pl.when((step > 0) & (step < last))
    def _():
        if samples > 1:
            norm_rows(h_ref, gain, bias, b_scr, jnp.maximum(group - 1, 0) * chunk, chunk)
        attend(nxt_scr)
        cur_scr[...] = nxt_scr[...]

    @pl.when(step == last)
    def _():
        attend(None)

    @pl.when((group == 0) & (step > 0))
    def _():
        o_ref[...] = (acc_scr[...] + old_ref[...].astype(F32) + bo_ref[layer : layer + 1].astype(F32)).astype(BF16)
        acc_scr[...] = jnp.zeros_like(acc_scr)


def call_attn(h, layer, norm, first, total, buf, text_len, ln_gain, ln_bias, mids, mid_specs, w_o, wo_lead, b_o, width, parts, flops):
    samples, tokens, ch = h.shape
    groups = ch // width
    now = lambda s, g: jnp.where(s < samples, g, groups - 1)
    old = lambda s, g: jnp.where(s < samples, jnp.where(g > 0, s, jnp.maximum(s - 1, 0)), samples - 1)
    lag = lambda s, g: jnp.where(s < samples, jnp.where(g > 0, g - 1, jnp.where(s > 0, groups - 1, 0)), groups - 1)
    full = lambda shape: pl.BlockSpec(shape, lambda s, g: (0,) * len(shape))
    lead = (None,) * len(wo_lead)
    in_specs = [
        pl.BlockSpec((None, tokens, ch), lambda s, g: (jnp.where(s + g == 0, 0, jnp.minimum(s + 1, samples - 1)), 0, 0)),
        pl.BlockSpec((None, tokens, ch), lambda s, g: (old(s, g), 0, 0)),
        full(ln_gain.shape), full(ln_bias.shape),
        *mid_specs(now, old, lag),
        pl.BlockSpec((*lead, width, ch), lambda s, g: (*wo_lead, lag(s, g), 0)), full(b_o.shape),
    ]
    args = [h, h, ln_gain, ln_bias, *mids, w_o, b_o]
    aliases = {}
    if buf is not None:
        in_specs.append(pl.BlockSpec(memory_space=pl.ANY))
        args.append(buf)
        aliases = {len(args) - 1: 0}
    return pl.pallas_call(
        functools.partial(attn_kernel, layer, norm, samples, groups, text_len),
        grid=(samples + 1, groups),
        in_specs=in_specs,
        out_specs=pl.BlockSpec((None, tokens, ch), lambda s, g: (first + old(s, g), 0, 0)),
        out_shape=jax.ShapeDtypeStruct((total, tokens, ch), BF16),
        scratch_shapes=[
            pltpu.VMEM((tokens, ch), BF16),
            pltpu.VMEM((tokens, ch), BF16),
            pltpu.VMEM((tokens, ch), F32),
            pltpu.VMEM((tokens, parts * width), BF16),
            pltpu.VMEM((tokens, parts * width), BF16),
        ],
        input_output_aliases=aliases,
        **params(2, flops, samples * (2 * (parts + 1) * ch * ch + 4 * tokens * ch)),
    )(*args)


def call_self(h, layer, first, total, buf, ln_gain, ln_bias, w_self, b_self):
    samples, tokens, ch = h.shape
    width = 256
    flops = samples * (2 * tokens * ch * ch * 4 + 4 * tokens * tokens * ch * 4)

    def mid_specs(now, old, lag):
        col = lambda j: pl.BlockSpec((None, None, ch, width), lambda s, g: (layer, j, 0, now(s, g)))
        return [col(0), col(1), col(2)]

    return call_attn(h, layer, 0, first, total, buf, 0, ln_gain, ln_bias, [w_self] * 3, mid_specs, w_self, (layer, 3),
                     b_self, width, 3, flops)


def call_cross(h, layer, text_len, k_text, v_text, ln_gain, ln_bias, w_q, w_o, b_cross):
    samples, tokens, ch = h.shape
    width = 256
    key_rows = k_text.shape[1]
    flops = samples * (2 * tokens * ch * ch * 2 + 4 * tokens * 128 * ch)

    def mid_specs(now, old, lag):
        txt = pl.BlockSpec((None, key_rows, width), lambda s, g: (old(s, g), 0, lag(s, g)))
        return [pl.BlockSpec((None, ch, width), lambda s, g: (layer, 0, now(s, g))), txt, txt]

    return call_attn(h, layer, 1, 0, samples, None, text_len, ln_gain, ln_bias, [w_q, k_text, v_text], mid_specs, w_o,
                     (layer,), b_cross, width, 1, flops)


def ff_kernel(layer, chunks, tiles, h_ref, gain_ref, bias_ref, wp_ref, wq_ref, bp_ref, bq_ref, w2_ref, b2_ref, o_ref, a_scr, acc_scr, *z_scrs):
    chunk = pl.program_id(1)
    step = pl.program_id(0) * chunks + chunk
    last = chunks * tiles
    rows = h_ref.shape[0]
    before = jnp.where(chunk > 0, chunk - 1, chunks - 1)

    @pl.when(step < chunks)
    def _():
        norm_all(
            h_ref, gain_ref[layer, 2:3].astype(F32), bias_ref[layer, 2:3].astype(F32), a_scr,
            acc_scr, b2_ref[layer : layer + 1].astype(F32), offset=step * rows,
        )

    def first_half(dst):
        at = pl.ds(pl.multiple_of(chunk * rows, rows), rows)
        act = a_scr[at, :]
        for n in range(0, dst.shape[1], 256):
            cols = slice(n, n + 256)
            p_val = (mm(act, wp_ref[:, cols]) + bp_ref[layer : layer + 1, cols].astype(F32)).astype(BF16).astype(F32)
            q_val = (mm(act, wq_ref[:, cols]) + bq_ref[layer : layer + 1, cols].astype(F32)).astype(BF16).astype(F32)
            gate = 0.5 * q_val * (1.0 + lax.erf(q_val * (2.0**-0.5)))
            dst[:, cols] = (p_val * gate).astype(BF16)

    def second_half(src):
        at = pl.ds(pl.multiple_of(before * rows, rows), rows)
        acc_scr[at, :] += mm(src[...], w2_ref[...])

    @pl.when(step == 0)
    def _():
        first_half(z_scrs[0])

    for parity in range(2):

        @pl.when((step > 0) & (step < last) & ((step & 1) == parity))
        def _():
            first_half(z_scrs[parity])
            second_half(z_scrs[1 - parity])

    @pl.when(step == last)
    def _():
        second_half(z_scrs[(last - 1) % 2])

    @pl.when((step > last - chunks) & (step <= last))
    def _():
        at = pl.ds(pl.multiple_of(before * rows, rows), rows)
        o_ref[...] = acc_scr[at, :].astype(BF16)


def call_ff(h, layer, first, samples, ln_gain, ln_bias, w1, b1, w2, b2):
    tokens, ch = h.shape[1:]
    ff_dim = w2.shape[1]
    width = 1024 if samples > 2 else 512
    tiles = ff_dim // width
    chunks = samples
    tile = lambda f: jnp.minimum(f, tiles - 1)
    lag_tile = lambda f, c: jnp.where(f < tiles, jnp.where(c > 0, f, jnp.maximum(f - 1, 0)), tiles - 1)
    done = lambda f, c: jnp.where(f < tiles, jnp.where(f == tiles - 1, jnp.maximum(c - 1, 0), 0), chunks - 1)
    full = lambda shape: pl.BlockSpec(shape, lambda f, c: (0,) * len(shape))
    flops = 6 * chunks * tokens * ch * ff_dim
    return pl.pallas_call(
        functools.partial(ff_kernel, layer, chunks, tiles),
        grid=(tiles + 1, chunks),
        in_specs=[
            pl.BlockSpec((None, tokens, ch), lambda f, c: (first + jnp.where(f == 0, c, chunks - 1), 0, 0)),
            full(ln_gain.shape),
            full(ln_bias.shape),
            pl.BlockSpec((None, ch, width), lambda f, c: (layer, 0, tile(f))),
            pl.BlockSpec((None, ch, width), lambda f, c: (layer, 0, tiles + tile(f))),
            pl.BlockSpec((b1.shape[0], width), lambda f, c: (0, tile(f))),
            pl.BlockSpec((b1.shape[0], width), lambda f, c: (0, tiles + tile(f))),
            pl.BlockSpec((None, width, ch), lambda f, c: (layer, lag_tile(f, c), 0)),
            full(b2.shape),
        ],
        out_specs=pl.BlockSpec((None, tokens, ch), lambda f, c: (done(f, c), 0, 0)),
        out_shape=jax.ShapeDtypeStruct((samples, tokens, ch), BF16),
        scratch_shapes=[
            pltpu.VMEM((chunks * tokens, ch), BF16),
            pltpu.VMEM((chunks * tokens, ch), F32),
            pltpu.VMEM((tokens, width), BF16),
            pltpu.VMEM((tokens, width), BF16),
        ],
        **params(2, flops, 6 * ch * ff_dim + 4 * chunks * tokens * ch),
        name="geglu_ff",
    )(h, ln_gain, ln_bias, w1, w1, b1, b1, w2, b2)


def out_kernel(first, per_dev, me_ref, *refs):
    n = (len(refs) - 6) // 2
    h_refs, x_refs = refs[:n], refs[n : 2 * n]
    w_ref, b_ref = refs[2 * n : 2 * n + 2]
    y_ref, h_scr, y_scr, sems = refs[-4:]
    rows = h_refs[0].shape[0]
    for k, ref in enumerate(h_refs):
        h_scr[k * rows : (k + 1) * rows, :] = ref[...]
    prod = mm(h_scr[...], w_ref[...]) + b_ref[...].astype(F32)
    copies = []
    for k, ref in enumerate(x_refs):
        y_scr[k] = (prod[k * rows : (k + 1) * rows] + ref[...].astype(F32)).astype(BF16)
    for k in range(n):
        place = per_dev * jnp.bitwise_xor(me_ref[0], k) + first + pl.program_id(0)
        copies.append(pltpu.make_async_copy(y_scr.at[k], y_ref.at[place], sems.at[k]))
        copies[-1].start()
    for copy in copies:
        copy.wait()


def call_out(me, first, per_dev, pieces, x, w_out, b_out, buf):
    samples, rows, ch = pieces[0].shape
    n = len(pieces)
    full = lambda shape: pl.BlockSpec(shape, lambda s, m: (0,) * len(shape))
    any_spec = pl.BlockSpec(memory_space=pl.ANY)

    def place(k):
        return pl.BlockSpec((None, rows, ch), lambda s, m: (per_dev * jnp.bitwise_xor(m[0], k) + first + s, 0, 0))

    in_specs = [pl.BlockSpec((None, rows, ch), lambda s, m: (s, 0, 0))] * n + [place(k) for k in range(n)]
    in_specs += [full((ch, ch)), full((1, ch))]
    args = [*pieces, *[x] * n, w_out, b_out]
    aliases = {}
    if buf is not None:
        in_specs.append(any_spec)
        args.append(buf)
        aliases = {len(args): 0}
    return pl.pallas_call(
        functools.partial(out_kernel, first, per_dev),
        grid_spec=pltpu.PrefetchScalarGridSpec(
            num_scalar_prefetch=1, grid=(samples,), in_specs=in_specs, out_specs=any_spec,
            scratch_shapes=[
                pltpu.VMEM((n * rows, ch), BF16), pltpu.VMEM((n, rows, ch), BF16), pltpu.SemaphoreType.DMA((n,)),
            ],
        ),
        out_shape=jax.ShapeDtypeStruct(x.shape, BF16),
        input_output_aliases=aliases,
        **params(1, samples * 2 * n * rows * ch * ch, 2 * ch * ch + samples * 6 * n * rows * ch),
        name="proj_out",
    )(me, *args)


def text_proj(ctx, w_kv):
    samples, length, dim = ctx.shape
    flat = ctx.reshape(samples * length, dim)
    return tuple(mm(flat, w_kv[j]).astype(BF16).reshape(samples, length, -1) for j in range(2))


def solution(mesh):
    n = mesh.shape["sp"]
    tok_spec = P("dp", "sp", None, None)
    ctx_spec = P("dp", None, None)
    replicated = P()

    def local_forward(latent, context, gn_gain, gn_bias, w_in, b_in, ln_gain, ln_bias, w_self, b_self, w_cross_q, w_cross_kv, w_cross_o, b_cross, w_ff1, b_ff1, w_ff2, b_ff2, w_out, b_out):
        batch, rows, columns, ch = latent.shape
        tokens = rows * columns
        layers = w_self.shape[0]
        per_dev = batch // n
        me = lax.axis_index("sp")
        x = latent.reshape(batch, tokens, ch)

        def swap(val, k):
            return lax.ppermute(val, "sp", [(i, i ^ k) for i in range(n)])


        pieces = []
        for first in range(0, per_dev, 2):
            take = lambda k: lax.dynamic_slice_in_dim(x, per_dev * jnp.bitwise_xor(me, k) + first, 2, 0)
            pieces.append([take(0)] + [swap(take(k), k) for k in range(1, n)])

        text_len = context.shape[1]
        ctx = lax.dynamic_slice_in_dim(context, per_dev * me, per_dev, 0)
        ctx = jnp.pad(ctx, ((0, 0), (0, -text_len % 16), (0, 0)))
        text = [text_proj(ctx, w_cross_kv[layer]) for layer in range(layers)]

        h = None
        for g, blocks in enumerate(pieces):
            part = call_in(blocks, gn_gain[None], gn_bias[None], w_in, b_in[None])
            h = call_self(part, 0, 2 * g, per_dev, h, ln_gain, ln_bias, w_self, b_self)
        for layer in range(layers):
            if layer:
                h = call_self(h, layer, 0, per_dev, None, ln_gain, ln_bias, w_self, b_self)
            h = call_cross(h, layer, text_len, *text[layer], ln_gain, ln_bias, w_cross_q, w_cross_o, b_cross)
            if layer < layers - 1:
                h = call_ff(h, layer, 0, per_dev, ln_gain, ln_bias, w_ff1, b_ff1, w_ff2, b_ff2)
        y = None
        me_arr = me.astype(jnp.int32).reshape(1)
        for first, count in ((0, 2), (2, 1), (3, 1)):
            part = call_ff(h, layers - 1, first, count, ln_gain, ln_bias, w_ff1, b_ff1, w_ff2, b_ff2)
            h, part = lax.optimization_barrier((h, part))
            back = [part[:, k * tokens : (k + 1) * tokens] for k in range(n)]
            back = [back[0]] + [swap(back[k], k) for k in range(1, n)]
            y = call_out(me_arr, first, per_dev, back, x, w_out, b_out[None], y)
        return y.reshape(latent.shape)

    in_specs = (tok_spec, ctx_spec) + (replicated,) * 18

    return jax.shard_map(local_forward, mesh=mesh, in_specs=in_specs, out_specs=tok_spec, check_vma=False)
```
